32 devices in a mesh: hst: 4 (over y, core), dev: 8 (over z, x).
Axes of the slice: x: 2, y: 2, z: 4, core: 2. Of those that a mesh axis runs over, the one named last changes fastest.
Arguments:
- hot_rows: bfloat16 [4096, 768], replicated, may hold values from -6 to 6
- cold_rows: bfloat16 [32768, 768], P(('hst', 'dev')), may hold values from -6 to 6
- hot_mask: int32 [65536], P(('hst', 'dev')), may hold values from 0 to 1, as said below
- hot_id: int32 [65536], P(('hst', 'dev')), may hold values from 0 to 4095
- cold_owner: int32 [65536], P(('hst', 'dev')), may hold values from 0 to 31, as said below
- cold_pos: int32 [65536], P(('hst', 'dev')), may hold values from 0 to 63, as said below
- cold_send: int32 [32, 2048], P(('hst', 'dev')), may hold values from 0 to 1023
- adjacency_one: int32 [65536, 15], P(('hst', 'dev')), may hold values from 0 to 2047
- adjacency_two: int32 [16384, 15], P(('hst', 'dev')), may hold values from 0 to 2303
- halo_send: int32 [32, 256], P(('hst', 'dev')), may hold values from 0 to 2047
- self_first: bfloat16 [768, 1024], replicated, may hold values from -0.21875 to 0.21875
- neigh_first: bfloat16 [768, 1024], replicated, may hold values from -0.21875 to 0.21875
- bn_gain: float32 [1024], replicated, may hold values from 0.1 to 1.9
- bn_shift: float32 [1024], replicated, may hold values from -3 to 3
- self_second: bfloat16 [1024, 153], replicated, may hold values from -0.1875 to 0.1875
- neigh_second: bfloat16 [1024, 153], replicated, may hold values from -0.1875 to 0.1875
Outputs:
- logits: float32 [16384, 153], P(('hst', 'dev'))
The draws below stay inside these ranges and needn't reach their ends.
Inputs may be any that keep to these rules, and one draw needn't show every extreme that they name: Each device has exactly 1536 nodes with hot_mask 0. `cold_owner`: for each device and owner, at most 64 of the device's nodes with hot_mask 0 name that owner; some owner is named by exactly 64 of them on every device. `cold_pos`: the nodes of one device with hot_mask 0 and the same owner have distinct slots.
All inputs are finite; a program needn't handle non-finite values.
Results may differ from the reference program's by a relative error of at most 0.003.
The reference program's roundings to bfloat16 on the way (of `features`, `first_mean`, `hidden`, `table` and `second_mean`) count: a program that leaves them out, or rounds other values in their place, can miss the bound.
Values may be sent and summed in bfloat16 or wider, within the bound.
A program may use at most 128 MiB of HBM per device.

```python
import math
import jax
import jax.numpy as jnp
import numpy as np
from jax import lax

F = 768
H = 1024
C = 153
L_DEV = 2048
COLD_DEV = 1024
HCAP = 32
HOT = 4096
K1 = 15
K2 = 15
COLD_NODES = 1536
B_DEV = 512
CAP = 64
NODES = 65536
TARGETS = 16384
COLD_ROWS = 32768
N_HST = 4
N_DEV = 8
DEVICES = 32


def cold_layout(key):
    base = jax.random.fold_in(key, 7)
    key_slots, key_nodes = jax.random.split(base)
    total_slots = DEVICES * CAP
    slot_index = jnp.arange(total_slots, dtype=jnp.int32)
    noise = jax.random.randint(key_slots, (DEVICES, total_slots), 0, 2 ** 19, dtype=jnp.int32)
    scores = noise * total_slots + slot_index[None, :]
    forced = (slot_index // CAP)[None, :] == ((jnp.arange(DEVICES, dtype=jnp.int32) + 1) % DEVICES)[:, None]
    scores = jnp.where(forced, slot_index[None, :] - total_slots, scores)
    chosen = jnp.argsort(scores, axis=1)[:, :COLD_NODES].astype(jnp.int32)
    owners = chosen // CAP
    positions = chosen % CAP
    node_noise = jax.random.randint(key_nodes, (DEVICES, L_DEV), 0, 2 ** 19, dtype=jnp.int32)
    node_scores = node_noise * L_DEV + jnp.arange(L_DEV, dtype=jnp.int32)[None, :]
    order = jnp.argsort(node_scores, axis=1)[:, :COLD_NODES].astype(jnp.int32)
    device_rows = jnp.broadcast_to(jnp.arange(DEVICES, dtype=jnp.int32)[:, None], order.shape)
    owner_full = jnp.zeros((DEVICES, L_DEV), jnp.int32).at[device_rows, order].set(owners)
    pos_full = jnp.zeros((DEVICES, L_DEV), jnp.int32).at[device_rows, order].set(positions)
    cold_flag = jnp.zeros((DEVICES, L_DEV), jnp.int32).at[device_rows, order].set(1)
    return (owner_full.reshape(-1), pos_full.reshape(-1), (1 - cold_flag).reshape(-1))


def draw_hot_mask(key, part):
    return cold_layout(key)[2]


def draw_cold_owner(key, part):
    return cold_layout(key)[0]


def draw_cold_pos(key, part):
    return cold_layout(key)[1]


def with_ends(drawn, rng, low, top_value):
    dims = drawn.shape
    place = [jax.random.randint(jax.random.fold_in(rng, axis), (), 0, dims[axis]) for axis in range(len(dims))]
    drawn = drawn.at[tuple(place)].set(low)
    longest = dims.index(max(dims))
    place[longest] = (place[longest] + 1) % dims[longest]
    return drawn.at[tuple(place)].set(top_value)


def shard_levels(rng, extent, pieces, low, high):
    level, own = 1.0, jax.random.fold_in(rng, 6)
    for dim, parts in pieces:
        draws = jnp.exp(jax.random.uniform(jax.random.fold_in(own, dim), (parts,), jnp.float32, low / len(pieces), high / len(pieces)))
        level = level * jnp.repeat(draws, extent[dim] // parts).reshape([-1 if axis == dim else 1 for axis in range(len(extent))])
    return level


def rank_table(count, slope):
    weights = [(1 << 20) // math.isqrt(standing ** slope) + 1 for standing in range(1, count + 1)]
    width = 1 + sum(weights) // (1 << 30)
    return np.cumsum(np.array([max(1, weight // width) for weight in weights]))


def ranked(own_key, dims, amount, skew):
    listing = rank_table(amount, skew)
    pick = jax.random.randint(jax.random.fold_in(own_key, 1), dims, 0, int(listing[amount - 1]))
    rank = jnp.searchsorted(jnp.asarray(listing, jnp.int32), pick, side="right")
    return jax.random.permutation(jax.random.fold_in(own_key, 2), amount)[rank].astype(jnp.int32)


def gaussian(rng, dims, deviation, bound, shards=(), kind=jnp.bfloat16):
    level = shard_levels(rng, dims, shards, -0.22, 0.18) if shards else 1.0
    values = jax.random.normal(rng, dims, jnp.float32) * deviation * level
    return jnp.minimum(jnp.maximum(values, -bound), bound).astype(kind)


def setup_inputs(seed: int = 0) -> dict:
    arg_keys = jax.random.split(jax.random.key(seed), 17)
    hot_rows = gaussian(arg_keys[0], (HOT, F), 1.0, 6.0)
    cold_rows = gaussian(arg_keys[1], (COLD_ROWS, F), 1.0, 6.0, ((0, 32),))
    hot_mask = draw_hot_mask(jax.random.fold_in(arg_keys[16], 71), 0)
    hot_id = with_ends(ranked(arg_keys[3], (NODES,), HOT, 2), jax.random.fold_in(arg_keys[3], 3), 0, HOT - 1).astype(jnp.int32)
    cold_owner = draw_cold_owner(jax.random.fold_in(arg_keys[16], 71), 0)
    cold_pos = draw_cold_pos(jax.random.fold_in(arg_keys[16], 71), 0)
    cold_send = with_ends(jax.random.randint(arg_keys[6], (DEVICES, DEVICES * CAP), 0, COLD_DEV), jax.random.fold_in(arg_keys[6], 1), 0, COLD_DEV - 1).astype(jnp.int32)
    adjacency_one = with_ends(jax.random.randint(arg_keys[7], (NODES, K1), 0, L_DEV), jax.random.fold_in(arg_keys[7], 1), 0, L_DEV - 1).astype(jnp.int32)
    adjacency_two = with_ends(jax.random.randint(arg_keys[8], (TARGETS, K2), 0, L_DEV + N_DEV * HCAP), jax.random.fold_in(arg_keys[8], 1), 0, (L_DEV + N_DEV * HCAP) - 1).astype(jnp.int32)
    halo_send = with_ends(jax.random.randint(arg_keys[9], (DEVICES, N_DEV * HCAP), 0, L_DEV), jax.random.fold_in(arg_keys[9], 1), 0, L_DEV - 1).astype(jnp.int32)
    self_first = gaussian(arg_keys[10], (F, H), F ** -0.5, 0.21875)
    neigh_first = gaussian(arg_keys[11], (F, H), F ** -0.5, 0.21875)
    bn_gain = jnp.clip(1.0 + 0.18 * jax.random.normal(arg_keys[12], (H,), jnp.float32), 0.1, 1.9)
    bn_shift = gaussian(arg_keys[13], (H,), 0.5, 3.0, (), jnp.float32)
    self_second = gaussian(arg_keys[14], (H, C), H ** -0.5, 0.1875)
    neigh_second = gaussian(arg_keys[15], (H, C), H ** -0.5, 0.1875)
    return {"hot_rows": hot_rows, "cold_rows": cold_rows, "hot_mask": hot_mask, "hot_id": hot_id, "cold_owner": cold_owner, "cold_pos": cold_pos, "cold_send": cold_send, "adjacency_one": adjacency_one, "adjacency_two": adjacency_two, "halo_send": halo_send, "self_first": self_first, "neigh_first": neigh_first, "bn_gain": bn_gain, "bn_shift": bn_shift, "self_second": self_second, "neigh_second": neigh_second}


epsilon = 1e-05

def gather_mean(table, neighbours, fanout):
    total = jnp.zeros((neighbours.shape[0], table.shape[1]), jnp.float32)
    for column in range(fanout):
        total = total + jnp.take(table, neighbours[:, column], axis=0).astype(jnp.float32)
    return (total / fanout).astype(jnp.bfloat16)

def reference(hot_rows, cold_rows, hot_mask, hot_id, cold_owner, cold_pos, cold_send, adjacency_one, adjacency_two, halo_send, self_first, neigh_first, bn_gain, bn_shift, self_second, neigh_second):
    devices = N_HST * N_DEV

    def first_layer(device):
        start = (device * L_DEV).astype(jnp.int32)
        mask_here = lax.dynamic_slice_in_dim(hot_mask, start, L_DEV)
        hot_here = lax.dynamic_slice_in_dim(hot_id, start, L_DEV)
        owner_here = lax.dynamic_slice_in_dim(cold_owner, start, L_DEV)
        pos_here = lax.dynamic_slice_in_dim(cold_pos, start, L_DEV)
        nbrs_here = lax.dynamic_slice_in_dim(adjacency_one, start, L_DEV)
        slot = cold_send[owner_here, (device * CAP + pos_here).astype(jnp.int32)]
        cold_feat = jnp.take(cold_rows, (owner_here * COLD_DEV + slot).astype(jnp.int32), axis=0)
        hot_feat = jnp.take(hot_rows, hot_here, axis=0)
        features = jnp.where(mask_here[:, None] == 1, hot_feat, cold_feat)
        first_mean = gather_mean(features, nbrs_here, K1)
        return jnp.dot(features, self_first, preferred_element_type=jnp.float32) + jnp.dot(first_mean, neigh_first, preferred_element_type=jnp.float32)
    hidden_pre = lax.map(first_layer, jnp.arange(devices, dtype=jnp.int32))
    mean = lax.optimization_barrier(jnp.mean(hidden_pre, axis=(0, 1)))
    variance = lax.optimization_barrier(jnp.mean(jnp.square(hidden_pre - mean), axis=(0, 1)))
    hidden = jax.nn.relu((hidden_pre - mean) * lax.rsqrt(variance + epsilon) * bn_gain + bn_shift).astype(jnp.bfloat16)
    sends = halo_send.reshape(devices, N_DEV, HCAP)

    def second_layer(device):
        group = device // N_DEV
        lane = device % N_DEV
        peers = (group * N_DEV + jnp.arange(N_DEV, dtype=jnp.int32)).astype(jnp.int32)
        picks = sends[peers, lane]
        boundary = hidden[peers[:, None], picks].reshape(N_DEV * HCAP, H)
        own = lax.dynamic_index_in_dim(hidden, device, 0, keepdims=False)
        table = jnp.concatenate([own, boundary], axis=0)
        nbrs_here = lax.dynamic_slice_in_dim(adjacency_two, (device * B_DEV).astype(jnp.int32), B_DEV)
        second_mean = gather_mean(table, nbrs_here, K2)
        return jnp.dot(own[:B_DEV], self_second, preferred_element_type=jnp.float32) + jnp.dot(second_mean, neigh_second, preferred_element_type=jnp.float32)
    logits = lax.map(second_layer, jnp.arange(devices, dtype=jnp.int32))
    return logits.reshape(devices * B_DEV, C)
```

```python
import functools

import jax
import jax.numpy as jnp
from jax import lax
from jax.experimental import pallas as pl
from jax.experimental.pallas import tpu as pltpu
from jax.sharding import PartitionSpec as P

epsilon = 1e-05
LANES = 128
GRANT = 48 * 1024 * 1024


def whole(shape):
    return pl.BlockSpec(shape, lambda *_: (0,) * len(shape))


def block_of(rows, wanted):
    while rows % wanted:
        wanted //= 2
    return wanted


def select_kernel(index_ref, rows_ref, out_ref):
    columns = lax.broadcasted_iota(jnp.int32, (index_ref.shape[0], rows_ref.shape[0]), 1)
    picks = jnp.where(index_ref[...] == columns, 1.0, 0.0).astype(jnp.bfloat16)
    out_ref[...] = jnp.dot(picks, rows_ref[...], preferred_element_type=jnp.float32).astype(out_ref.dtype)


def select_rows(rows, index):
    count, width = index.shape[0], rows.shape[1]
    step = block_of(count, 512)
    return pl.pallas_call(
        select_kernel,
        grid=(count // step,),
        in_specs=[pl.BlockSpec((step, 1), lambda i: (i, 0)), whole(rows.shape)],
        out_specs=pl.BlockSpec((step, width), lambda i: (i, 0)),
        out_shape=jax.ShapeDtypeStruct((count, width), rows.dtype),
        compiler_params=pltpu.CompilerParams(vmem_limit_bytes=GRANT),
        name="select_rows",
    )(index[:, None], rows)


def count_kernel(index_ref, out_ref):
    rows, fanout = index_ref.shape
    width = out_ref.shape[1]
    part = 16

    def some_rows(step, carry):
        here = pl.ds(pl.multiple_of(step * part, part), part)
        index = index_ref[here, :]
        lane = lax.broadcasted_iota(jnp.int32, (part, LANES), 1)
        spread = [jnp.broadcast_to(index[:, k : k + 1], (part, LANES)) for k in range(fanout)]
        for tile in range(width // LANES):
            columns = lane + tile * LANES
            total = jnp.zeros((part, LANES), jnp.float32)
            for k in range(fanout):
                total = total + jnp.where(spread[k] == columns, 1.0, 0.0)
            out_ref[here, tile * LANES : (tile + 1) * LANES] = total.astype(jnp.bfloat16)
        return carry

    lax.fori_loop(0, rows // part, some_rows, 0)


def count_matrix(index, width):
    rows, fanout = index.shape
    step = block_of(rows, 512)
    return pl.pallas_call(
        count_kernel,
        grid=(rows // step,),
        in_specs=[pl.BlockSpec((step, fanout), lambda i: (i, 0))],
        out_specs=pl.BlockSpec((step, width), lambda i: (i, 0)),
        out_shape=jax.ShapeDtypeStruct((rows, width), jnp.bfloat16),
        compiler_params=pltpu.CompilerParams(vmem_limit_bytes=16 * 1024 * 1024),
        cost_estimate=pl.CostEstimate(
            flops=rows * width * fanout * 150, bytes_accessed=rows * width * 2, transcendentals=0
        ),
        name="count_matrix",
    )(index)


def first_kernel(blocks, fanout, arrived_ref, place_ref, hot_ref, counts_ref, self_ref, neigh_ref,
                 pre_ref, stats_ref, features):
    step = pl.program_id(0)
    rows = place_ref.shape[0]

    @pl.when(step < blocks)
    def _():
        cold = jnp.dot(place_ref[...], arrived_ref[...], preferred_element_type=jnp.float32)
        here = pl.ds(pl.multiple_of(step * rows, rows), rows)
        features[here, :] = cold.astype(jnp.bfloat16) + hot_ref[...]

    @pl.when(step >= blocks)
    def _():
        here = pl.ds(pl.multiple_of((step - blocks) * rows, rows), rows)
        total = jnp.dot(counts_ref[...], features[...], preferred_element_type=jnp.float32)
        mean = (total / fanout).astype(jnp.bfloat16)
        pre = jnp.dot(features[here, :], self_ref[...], preferred_element_type=jnp.float32)
        pre = pre + jnp.dot(mean, neigh_ref[...], preferred_element_type=jnp.float32)
        pre_ref[...] = pre
        both = jnp.concatenate(
            [jnp.sum(pre, axis=0, keepdims=True), jnp.sum(pre * pre, axis=0, keepdims=True)], axis=0
        )

        @pl.when(step == blocks)
        def _():
            stats_ref[...] = both

        @pl.when(step > blocks)
        def _():
            stats_ref[...] += both


def first_layer(arrived, place, hot_feat, counts, self_first, neigh_first, fanout):
    nodes, width = hot_feat.shape
    units = self_first.shape[1]
    step = block_of(nodes, 512)
    blocks = nodes // step
    early = lambda i: (jnp.minimum(i, blocks - 1), 0)
    late = lambda i: (jnp.maximum(i - blocks, 0), 0)
    return pl.pallas_call(
        functools.partial(first_kernel, blocks, fanout),
        grid=(2 * blocks,),
        in_specs=[
            whole(arrived.shape),
            pl.BlockSpec((step, place.shape[1]), early),
            pl.BlockSpec((step, width), early),
            pl.BlockSpec((step, counts.shape[1]), late),
            whole(self_first.shape),
            whole(neigh_first.shape),
        ],
        out_specs=[pl.BlockSpec((step, units), late), whole((2, units))],
        out_shape=[
            jax.ShapeDtypeStruct((nodes, units), jnp.float32),
            jax.ShapeDtypeStruct((2, units), jnp.float32),
        ],
        scratch_shapes=[pltpu.VMEM((nodes, width), jnp.bfloat16)],
        compiler_params=pltpu.CompilerParams(vmem_limit_bytes=GRANT),
        name="first_layer",
    )(arrived, place, hot_feat, counts, self_first, neigh_first)


def stats_kernel(hosts, within, own_ref, out_ref, near, far, part, send_near, recv_near, send_far, recv_far):
    host, lane = lax.axis_index("hst"), lax.axis_index("dev")
    barrier = pltpu.get_barrier_semaphore()
    for away in range(1, within):
        pl.semaphore_signal(barrier, inc=1, device_id={"dev": lax.rem(lane + away, within)},
                            device_id_type=pl.DeviceIdType.MESH)
    for away in range(1, hosts):
        pl.semaphore_signal(barrier, inc=1, device_id={"hst": lax.rem(host + away, hosts)},
                            device_id_type=pl.DeviceIdType.MESH)
    pl.semaphore_wait(barrier, within + hosts - 2)

    def exchange(source, slots, axis, me, size, send, recv):
        copies = []
        for away in range(1, size):
            copy = pltpu.make_async_remote_copy(
                src_ref=source, dst_ref=slots.at[away - 1], send_sem=send.at[away - 1],
                recv_sem=recv.at[away - 1], device_id={axis: lax.rem(me + away, size)},
                device_id_type=pl.DeviceIdType.MESH,
            )
            copy.start()
            copies.append(copy)
        for copy in copies:
            copy.wait()
        total = source[...]
        for away in range(1, size):
            total = total + slots[away - 1]
        return total

    part[...] = exchange(own_ref, near, "dev", lane, within, send_near, recv_near)
    out_ref[...] = exchange(part, far, "hst", host, hosts, send_far, recv_far)


def sum_stats(own, hosts, within):
    return pl.pallas_call(
        functools.partial(stats_kernel, hosts, within),
        in_specs=[pl.BlockSpec(memory_space=pltpu.VMEM)],
        out_specs=pl.BlockSpec(memory_space=pltpu.VMEM),
        out_shape=jax.ShapeDtypeStruct(own.shape, own.dtype),
        scratch_shapes=[
            pltpu.VMEM((within - 1,) + own.shape, own.dtype),
            pltpu.VMEM((hosts - 1,) + own.shape, own.dtype),
            pltpu.VMEM(own.shape, own.dtype),
            pltpu.SemaphoreType.DMA((within - 1,)),
            pltpu.SemaphoreType.DMA((within - 1,)),
            pltpu.SemaphoreType.DMA((hosts - 1,)),
            pltpu.SemaphoreType.DMA((hosts - 1,)),
        ],
        compiler_params=pltpu.CompilerParams(collective_id=0, has_side_effects=True),
        name="sum_stats",
    )(own)


def norm_kernel(total_rows, pre_ref, stats_ref, gain_ref, shift_ref, picks_ref, hidden_ref, boundary_ref, held):
    step = pl.program_id(0)
    mean = stats_ref[0:1, :] / total_rows
    variance = stats_ref[1:2, :] / total_rows - mean * mean
    scale = lax.rsqrt(variance + epsilon)
    hidden = jnp.maximum((pre_ref[...] - mean) * scale * gain_ref[...] + shift_ref[...], 0.0)
    hidden = hidden.astype(jnp.bfloat16)
    hidden_ref[...] = hidden
    picked = jnp.dot(picks_ref[...], hidden, preferred_element_type=jnp.float32)

    @pl.when(step == 0)
    def _():
        held[...] = picked

    @pl.when(step > 0)
    def _():
        held[...] += picked

    @pl.when(step == pl.num_programs(0) - 1)
    def _():
        boundary_ref[...] = held[...].astype(jnp.bfloat16)


def norm_layer(pre, stats, gain, shift, picks, total_rows):
    nodes, units = pre.shape
    step = block_of(nodes, 512)
    edge = picks.shape[0]
    return pl.pallas_call(
        functools.partial(norm_kernel, total_rows),
        grid=(nodes // step,),
        in_specs=[
            pl.BlockSpec((step, units), lambda i: (i, 0)),
            whole(stats.shape),
            whole((1, units)),
            whole((1, units)),
            pl.BlockSpec((edge, step), lambda i: (0, i)),
        ],
        out_specs=[pl.BlockSpec((step, units), lambda i: (i, 0)), whole((edge, units))],
        out_shape=[
            jax.ShapeDtypeStruct((nodes, units), jnp.bfloat16),
            jax.ShapeDtypeStruct((edge, units), jnp.bfloat16),
        ],
        scratch_shapes=[pltpu.VMEM((edge, units), jnp.float32)],
        compiler_params=pltpu.CompilerParams(vmem_limit_bytes=GRANT),
        name="norm_layer",
    )(pre, stats, gain[None, :], shift[None, :], picks)


def last_kernel(within, fanout, boundary_ref, hidden_ref, counts_ref, self_ref, neigh_ref, out_ref,
                received, send, recv, own_sem):
    lane = lax.axis_index("dev")
    nodes = hidden_ref.shape[0]
    targets = counts_ref.shape[0]
    slots = boundary_ref.shape[0] // within
    barrier = pltpu.get_barrier_semaphore()
    for away in range(1, within):
        pl.semaphore_signal(barrier, inc=1, device_id={"dev": lax.rem(lane + away, within)},
                            device_id_type=pl.DeviceIdType.MESH)
    pl.semaphore_wait(barrier, within - 1)
    mine = pl.ds(pl.multiple_of(lane * slots, slots), slots)
    copies = []
    for away in range(1, within):
        peer = lax.rem(lane + away, within)
        copy = pltpu.make_async_remote_copy(
            src_ref=boundary_ref.at[pl.ds(pl.multiple_of(peer * slots, slots), slots)],
            dst_ref=received.at[mine],
            send_sem=send.at[away - 1], recv_sem=recv.at[away - 1], device_id={"dev": peer},
            device_id_type=pl.DeviceIdType.MESH,
        )
        copy.start()
        copies.append(copy)
    own = pltpu.make_async_copy(boundary_ref.at[mine], received.at[mine], own_sem)
    own.start()
    total = jnp.dot(counts_ref[:, :nodes], hidden_ref[...], preferred_element_type=jnp.float32)
    scores = jnp.dot(hidden_ref[:targets, :], self_ref[...], preferred_element_type=jnp.float32)
    own.wait()
    for copy in copies:
        copy.wait()
    total = total + jnp.dot(counts_ref[:, nodes:], received[...], preferred_element_type=jnp.float32)
    mean = (total / fanout).astype(jnp.bfloat16)
    out_ref[...] = scores + jnp.dot(mean, neigh_ref[...], preferred_element_type=jnp.float32)


def last_layer(boundary, hidden, counts, self_second, neigh_second, within, fanout):
    return pl.pallas_call(
        functools.partial(last_kernel, within, fanout),
        in_specs=[pl.BlockSpec(memory_space=pltpu.VMEM)] * 5,
        out_specs=pl.BlockSpec(memory_space=pltpu.VMEM),
        out_shape=jax.ShapeDtypeStruct((counts.shape[0], self_second.shape[1]), jnp.float32),
        scratch_shapes=[
            pltpu.VMEM(boundary.shape, boundary.dtype),
            pltpu.SemaphoreType.DMA((within - 1,)),
            pltpu.SemaphoreType.DMA((within - 1,)),
            pltpu.SemaphoreType.DMA,
        ],
        compiler_params=pltpu.CompilerParams(
            collective_id=1, has_side_effects=True, vmem_limit_bytes=GRANT
        ),
        name="last_layer",
    )(boundary, hidden, counts, self_second, neigh_second)


def local(
    hot_rows,
    cold_rows,
    hot_mask,
    hot_id,
    cold_owner,
    cold_pos,
    cold_send,
    adjacency_one,
    adjacency_two,
    halo_send,
    self_first,
    neigh_first,
    bn_gain,
    bn_shift,
    self_second,
    neigh_second,
):
    hosts = lax.axis_size("hst")
    within = lax.axis_size("dev")
    nodes = hot_mask.shape[0]
    outgoing = select_rows(cold_rows, cold_send[0])
    slots = outgoing.shape[0] // (hosts * within)
    arrived = lax.all_to_all(outgoing, ("hst", "dev"), split_axis=0, concat_axis=0, tiled=True)

    hot_feat = jnp.where(
        hot_mask[:, None] == 1, hot_rows.at[hot_id].get(mode="promise_in_bounds"), 0
    )
    source = jnp.where(hot_mask == 1, -1, cold_owner * slots + cold_pos)
    place = count_matrix(source[:, None], outgoing.shape[0])
    counts_one = count_matrix(adjacency_one, nodes)
    counts_two = count_matrix(adjacency_two, nodes + halo_send.shape[1])
    picks = count_matrix(halo_send[0][:, None], nodes)

    pre, own = first_layer(
        arrived, place, hot_feat, counts_one, self_first, neigh_first, adjacency_one.shape[1]
    )
    stats = sum_stats(own, hosts, within)
    hidden, boundary = norm_layer(pre, stats, bn_gain, bn_shift, picks, nodes * hosts * within)
    return last_layer(
        boundary, hidden, counts_two, self_second, neigh_second, within, adjacency_two.shape[1]
    )


def solution(mesh):
    placed = (
        P(),
        P(("hst", "dev"), None),
        P(("hst", "dev")),
        P(("hst", "dev")),
        P(("hst", "dev")),
        P(("hst", "dev")),
        P(("hst", "dev"), None),
        P(("hst", "dev"), None),
        P(("hst", "dev"), None),
        P(("hst", "dev"), None),
        P(),
        P(),
        P(),
        P(),
        P(),
        P(),
    )
    return jax.shard_map(
        local, mesh=mesh, in_specs=placed, out_specs=P(("hst", "dev"), None), check_vma=False
    )
```

```python
import functools

import jax
import jax.numpy as jnp
from jax import lax
from jax.experimental import pallas as pl
from jax.experimental.pallas import tpu as pltpu
from jax.sharding import PartitionSpec as P

epsilon = 1e-05
LANES = 128
GRANT = 48 * 1024 * 1024


def whole(shape):
    return pl.BlockSpec(shape, lambda *_: (0,) * len(shape))


def block_of(rows, wanted):
    while rows % wanted:
        wanted //= 2
    return wanted


def one_hot(index, width):
    columns = lax.broadcasted_iota(jnp.int32, (index.shape[0], width), 1)
    return jnp.where(index == columns, 1.0, 0.0).astype(jnp.bfloat16)


def select_kernel(index_ref, rows_ref, out_ref):
    picks = one_hot(index_ref[...], rows_ref.shape[0])
    out_ref[...] = jnp.dot(picks, rows_ref[...], preferred_element_type=jnp.float32).astype(out_ref.dtype)


def select_rows(rows, index):
    count, width = index.shape[0], rows.shape[1]
    step = block_of(count, 512)
    return pl.pallas_call(
        select_kernel,
        grid=(count // step,),
        in_specs=[pl.BlockSpec((step, 1), lambda i: (i, 0)), whole(rows.shape)],
        out_specs=pl.BlockSpec((step, width), lambda i: (i, 0)),
        out_shape=jax.ShapeDtypeStruct((count, width), rows.dtype),
        compiler_params=pltpu.CompilerParams(vmem_limit_bytes=GRANT),
        name="select_rows",
    )(index[:, None], rows)


def count_kernel(index_ref, out_ref):
    rows, fanout = index_ref.shape
    width = out_ref.shape[1]
    part = 16

    def some_rows(step, carry):
        here = pl.ds(pl.multiple_of(step * part, part), part)
        index = index_ref[here, :]
        lane = lax.broadcasted_iota(jnp.int32, (part, LANES), 1).astype(jnp.int16)
        spread = [
            jnp.broadcast_to(index[:, k : k + 1], (part, LANES)).astype(jnp.int16) for k in range(fanout)
        ]
        one, none = jnp.ones((part, LANES), jnp.bfloat16), jnp.zeros((part, LANES), jnp.bfloat16)
        for tile in range(width // LANES):
            columns = lane + jnp.int16(tile * LANES)
            total = none
            for k in range(fanout):
                total = total + jnp.where(spread[k] == columns, one, none)
            out_ref[here, tile * LANES : (tile + 1) * LANES] = total
        return carry

    lax.fori_loop(0, rows // part, some_rows, 0)


def count_matrix(index, width):
    rows, fanout = index.shape
    step = block_of(rows, 512)
    return pl.pallas_call(
        count_kernel,
        grid=(rows // step,),
        in_specs=[pl.BlockSpec((step, fanout), lambda i: (i, 0))],
        out_specs=pl.BlockSpec((step, width), lambda i: (i, 0)),
        out_shape=jax.ShapeDtypeStruct((rows, width), jnp.bfloat16),
        compiler_params=pltpu.CompilerParams(vmem_limit_bytes=16 * 1024 * 1024),
        cost_estimate=pl.CostEstimate(
            flops=rows * width * fanout * 100, bytes_accessed=rows * width * 2, transcendentals=0
        ),
        name="count_matrix",
    )(index)


def first_kernel(blocks, fanout, arrived_ref, place_ref, hot_ref, counts_ref, self_ref, neigh_ref,
                 pre_ref, stats_ref, features):
    step = pl.program_id(0)
    rows = place_ref.shape[0]

    @pl.when(step < blocks)
    def _():
        place = one_hot(place_ref[...], arrived_ref.shape[0])
        cold = jnp.dot(place, arrived_ref[...], preferred_element_type=jnp.float32)
        here = pl.ds(pl.multiple_of(step * rows, rows), rows)
        features[here, :] = cold.astype(jnp.bfloat16) + hot_ref[...]

    @pl.when(step >= blocks)
    def _():
        here = pl.ds(pl.multiple_of((step - blocks) * rows, rows), rows)
        total = jnp.dot(counts_ref[...], features[...], preferred_element_type=jnp.float32)
        mean = (total / fanout).astype(jnp.bfloat16)
        pre = jnp.dot(features[here, :], self_ref[...], preferred_element_type=jnp.float32)
        pre = pre + jnp.dot(mean, neigh_ref[...], preferred_element_type=jnp.float32)
        pre_ref[...] = pre
        both = jnp.concatenate(
            [jnp.sum(pre, axis=0, keepdims=True), jnp.sum(pre * pre, axis=0, keepdims=True)], axis=0
        )

        @pl.when(step == blocks)
        def _():
            stats_ref[...] = both

        @pl.when(step > blocks)
        def _():
            stats_ref[...] += both


def first_layer(arrived, place, hot_feat, counts, self_first, neigh_first, fanout):
    nodes, width = hot_feat.shape
    units = self_first.shape[1]
    step = block_of(nodes, 512)
    blocks = nodes // step
    early = lambda i: (jnp.minimum(i, blocks - 1), 0)
    late = lambda i: (jnp.maximum(i - blocks, 0), 0)
    return pl.pallas_call(
        functools.partial(first_kernel, blocks, fanout),
        grid=(2 * blocks,),
        in_specs=[
            whole(arrived.shape),
            pl.BlockSpec((step, place.shape[1]), early),
            pl.BlockSpec((step, width), early),
            pl.BlockSpec((step, counts.shape[1]), late),
            whole(self_first.shape),
            whole(neigh_first.shape),
        ],
        out_specs=[pl.BlockSpec((step, units), late), whole((2, units))],
        out_shape=[
            jax.ShapeDtypeStruct((nodes, units), jnp.float32),
            jax.ShapeDtypeStruct((2, units), jnp.float32),
        ],
        scratch_shapes=[pltpu.VMEM((nodes, width), jnp.bfloat16)],
        compiler_params=pltpu.CompilerParams(vmem_limit_bytes=GRANT),
        name="first_layer",
    )(arrived, place, hot_feat, counts, self_first, neigh_first)


def stats_kernel(hosts, within, own_ref, out_ref, near, far, part, send_near, recv_near, send_far, recv_far):
    host, lane = lax.axis_index("hst"), lax.axis_index("dev")
    barrier = pltpu.get_barrier_semaphore()
    for away in range(1, within):
        pl.semaphore_signal(barrier, inc=1, device_id={"dev": lax.rem(lane + away, within)},
                            device_id_type=pl.DeviceIdType.MESH)
    for away in range(1, hosts):
        pl.semaphore_signal(barrier, inc=1, device_id={"hst": lax.rem(host + away, hosts)},
                            device_id_type=pl.DeviceIdType.MESH)
    pl.semaphore_wait(barrier, within + hosts - 2)

    def exchange(source, slots, axis, me, size, send, recv):
        copies = []
        for away in range(1, size):
            copy = pltpu.make_async_remote_copy(
                src_ref=source, dst_ref=slots.at[away - 1], send_sem=send.at[away - 1],
                recv_sem=recv.at[away - 1], device_id={axis: lax.rem(me + away, size)},
                device_id_type=pl.DeviceIdType.MESH,
            )
            copy.start()
            copies.append(copy)
        for copy in copies:
            copy.wait()
        total = source[...]
        for away in range(1, size):
            total = total + slots[away - 1]
        return total

    part[...] = exchange(own_ref, near, "dev", lane, within, send_near, recv_near)
    out_ref[...] = exchange(part, far, "hst", host, hosts, send_far, recv_far)


def sum_stats(own, hosts, within):
    return pl.pallas_call(
        functools.partial(stats_kernel, hosts, within),
        in_specs=[pl.BlockSpec(memory_space=pltpu.VMEM)],
        out_specs=pl.BlockSpec(memory_space=pltpu.VMEM),
        out_shape=jax.ShapeDtypeStruct(own.shape, own.dtype),
        scratch_shapes=[
            pltpu.VMEM((within - 1,) + own.shape, own.dtype),
            pltpu.VMEM((hosts - 1,) + own.shape, own.dtype),
            pltpu.VMEM(own.shape, own.dtype),
            pltpu.SemaphoreType.DMA((within - 1,)),
            pltpu.SemaphoreType.DMA((within - 1,)),
            pltpu.SemaphoreType.DMA((hosts - 1,)),
            pltpu.SemaphoreType.DMA((hosts - 1,)),
        ],
        compiler_params=pltpu.CompilerParams(collective_id=0, has_side_effects=True),
        name="sum_stats",
    )(own)


def norm_kernel(total_rows, pre_ref, stats_ref, gain_ref, shift_ref, picks_ref, hidden_ref, boundary_ref, held):
    step = pl.program_id(0)
    mean = stats_ref[0:1, :] / total_rows
    variance = stats_ref[1:2, :] / total_rows - mean * mean
    scale = lax.rsqrt(variance + epsilon)
    hidden = jnp.maximum((pre_ref[...] - mean) * scale * gain_ref[...] + shift_ref[...], 0.0)
    hidden = hidden.astype(jnp.bfloat16)
    hidden_ref[...] = hidden
    picks = one_hot(picks_ref[...] - step * hidden.shape[0], hidden.shape[0])
    picked = jnp.dot(picks, hidden, preferred_element_type=jnp.float32)

    @pl.when(step == 0)
    def _():
        held[...] = picked

    @pl.when(step > 0)
    def _():
        held[...] += picked

    @pl.when(step == pl.num_programs(0) - 1)
    def _():
        boundary_ref[...] = held[...].astype(jnp.bfloat16)


def norm_layer(pre, stats, gain, shift, picks, total_rows):
    nodes, units = pre.shape
    step = block_of(nodes, 512)
    edge = picks.shape[0]
    return pl.pallas_call(
        functools.partial(norm_kernel, total_rows),
        grid=(nodes // step,),
        in_specs=[
            pl.BlockSpec((step, units), lambda i: (i, 0)),
            whole(stats.shape),
            whole((1, units)),
            whole((1, units)),
            whole((edge, 1)),
        ],
        out_specs=[pl.BlockSpec((step, units), lambda i: (i, 0)), whole((edge, units))],
        out_shape=[
            jax.ShapeDtypeStruct((nodes, units), jnp.bfloat16),
            jax.ShapeDtypeStruct((edge, units), jnp.bfloat16),
        ],
        scratch_shapes=[pltpu.VMEM((edge, units), jnp.float32)],
        compiler_params=pltpu.CompilerParams(vmem_limit_bytes=GRANT),
        name="norm_layer",
    )(pre, stats, gain[None, :], shift[None, :], picks)


def last_kernel(within, fanout, boundary_ref, hidden_ref, counts_ref, self_ref, neigh_ref, out_ref,
                received, send, recv, own_sem):
    lane = lax.axis_index("dev")
    nodes = hidden_ref.shape[0]
    targets = counts_ref.shape[0]
    slots = boundary_ref.shape[0] // within
    barrier = pltpu.get_barrier_semaphore()
    for away in range(1, within):
        pl.semaphore_signal(barrier, inc=1, device_id={"dev": lax.rem(lane + away, within)},
                            device_id_type=pl.DeviceIdType.MESH)
    pl.semaphore_wait(barrier, within - 1)
    mine = pl.ds(pl.multiple_of(lane * slots, slots), slots)
    copies = []
    for away in range(1, within):
        peer = lax.rem(lane + away, within)
        copy = pltpu.make_async_remote_copy(
            src_ref=boundary_ref.at[pl.ds(pl.multiple_of(peer * slots, slots), slots)],
            dst_ref=received.at[mine],
            send_sem=send.at[away - 1], recv_sem=recv.at[away - 1], device_id={"dev": peer},
            device_id_type=pl.DeviceIdType.MESH,
        )
        copy.start()
        copies.append(copy)
    own = pltpu.make_async_copy(boundary_ref.at[mine], received.at[mine], own_sem)
    own.start()
    total = jnp.dot(counts_ref[:, :nodes], hidden_ref[...], preferred_element_type=jnp.float32)
    scores = jnp.dot(hidden_ref[:targets, :], self_ref[...], preferred_element_type=jnp.float32)
    own.wait()
    for copy in copies:
        copy.wait()
    total = total + jnp.dot(counts_ref[:, nodes:], received[...], preferred_element_type=jnp.float32)
    mean = (total / fanout).astype(jnp.bfloat16)
    out_ref[...] = scores + jnp.dot(mean, neigh_ref[...], preferred_element_type=jnp.float32)


def last_layer(boundary, hidden, counts, self_second, neigh_second, within, fanout):
    return pl.pallas_call(
        functools.partial(last_kernel, within, fanout),
        in_specs=[pl.BlockSpec(memory_space=pltpu.VMEM)] * 5,
        out_specs=pl.BlockSpec(memory_space=pltpu.VMEM),
        out_shape=jax.ShapeDtypeStruct((counts.shape[0], self_second.shape[1]), jnp.float32),
        scratch_shapes=[
            pltpu.VMEM(boundary.shape, boundary.dtype),
            pltpu.SemaphoreType.DMA((within - 1,)),
            pltpu.SemaphoreType.DMA((within - 1,)),
            pltpu.SemaphoreType.DMA,
        ],
        compiler_params=pltpu.CompilerParams(
            collective_id=1, has_side_effects=True, vmem_limit_bytes=GRANT
        ),
        name="last_layer",
    )(boundary, hidden, counts, self_second, neigh_second)


def local(
    hot_rows,
    cold_rows,
    hot_mask,
    hot_id,
    cold_owner,
    cold_pos,
    cold_send,
    adjacency_one,
    adjacency_two,
    halo_send,
    self_first,
    neigh_first,
    bn_gain,
    bn_shift,
    self_second,
    neigh_second,
):
    hosts = lax.axis_size("hst")
    within = lax.axis_size("dev")
    nodes = hot_mask.shape[0]
    outgoing = select_rows(cold_rows, cold_send[0])
    slots = outgoing.shape[0] // (hosts * within)
    arrived = lax.all_to_all(outgoing, ("hst", "dev"), split_axis=0, concat_axis=0, tiled=True)

    hot_feat = jnp.where(
        hot_mask[:, None] == 1, hot_rows.at[hot_id].get(mode="promise_in_bounds"), 0
    )
    source = jnp.where(hot_mask == 1, -1, cold_owner * slots + cold_pos)
    place = source[:, None]
    counts_one = count_matrix(adjacency_one, nodes)
    counts_two = count_matrix(adjacency_two, nodes + halo_send.shape[1])
    picks = halo_send[0][:, None]

    pre, own = first_layer(
        arrived, place, hot_feat, counts_one, self_first, neigh_first, adjacency_one.shape[1]
    )
    stats = sum_stats(own, hosts, within)
    hidden, boundary = norm_layer(pre, stats, bn_gain, bn_shift, picks, nodes * hosts * within)
    return last_layer(
        boundary, hidden, counts_two, self_second, neigh_second, within, adjacency_two.shape[1]
    )


def solution(mesh):
    placed = (
        P(),
        P(("hst", "dev"), None),
        P(("hst", "dev")),
        P(("hst", "dev")),
        P(("hst", "dev")),
        P(("hst", "dev")),
        P(("hst", "dev"), None),
        P(("hst", "dev"), None),
        P(("hst", "dev"), None),
        P(("hst", "dev"), None),
        P(),
        P(),
        P(),
        P(),
        P(),
        P(),
    )
    return jax.shard_map(
        local, mesh=mesh, in_specs=placed, out_specs=P(("hst", "dev"), None), check_vma=False
    )
```

```python
import functools

import jax
import jax.numpy as jnp
from jax import lax
from jax.experimental import pallas as pl
from jax.experimental.pallas import tpu as pltpu
from jax.sharding import PartitionSpec as P

epsilon = 1e-05
LANES = 128
MIB = 1024 * 1024


def whole(shape):
    return pl.BlockSpec(shape, lambda *_: (0,) * len(shape))


def block_of(rows, wanted):
    while rows % wanted:
        wanted //= 2
    return wanted


def one_hot(index, width):
    columns = lax.broadcasted_iota(jnp.int32, (index.shape[0], width), 1)
    return jnp.where(index == columns, 1.0, 0.0).astype(jnp.bfloat16)


def select_kernel(index_ref, rows_ref, out_ref):
    picks = one_hot(index_ref[...], rows_ref.shape[0])
    out_ref[...] = jnp.dot(picks, rows_ref[...], preferred_element_type=jnp.float32).astype(out_ref.dtype)


def select_rows(rows, index):
    count, width = index.shape[0], rows.shape[1]
    step = block_of(count, 512)
    return pl.pallas_call(
        select_kernel,
        grid=(count // step,),
        in_specs=[pl.BlockSpec((step, 1), lambda i: (i, 0)), whole(rows.shape)],
        out_specs=pl.BlockSpec((step, width), lambda i: (i, 0)),
        out_shape=jax.ShapeDtypeStruct((count, width), rows.dtype),
        compiler_params=pltpu.CompilerParams(vmem_limit_bytes=16 * MIB),
        name="select_rows",
    )(index[:, None], rows)


def count_kernel(index_ref, out_ref):
    rows, fanout = index_ref.shape
    width = out_ref.shape[1]
    part = 16

    def some_rows(step, carry):
        here = pl.ds(pl.multiple_of(step * part, part), part)
        index = index_ref[here, :]
        lane = lax.broadcasted_iota(jnp.int32, (part, LANES), 1).astype(jnp.int16)
        spread = [
            jnp.broadcast_to(index[:, k : k + 1], (part, LANES)).astype(jnp.int16) for k in range(fanout)
        ]
        one, none = jnp.ones((part, LANES), jnp.bfloat16), jnp.zeros((part, LANES), jnp.bfloat16)
        for tile in range(width // LANES):
            columns = lane + jnp.int16(tile * LANES)
            total = none
            for k in range(fanout):
                total = total + jnp.where(spread[k] == columns, one, none)
            out_ref[here, tile * LANES : (tile + 1) * LANES] = total
        return carry

    lax.fori_loop(0, rows // part, some_rows, 0)


def count_matrix(index, width):
    rows, fanout = index.shape
    step = block_of(rows, 512)
    return pl.pallas_call(
        count_kernel,
        grid=(rows // step,),
        in_specs=[pl.BlockSpec((step, fanout), lambda i: (i, 0))],
        out_specs=pl.BlockSpec((step, width), lambda i: (i, 0)),
        out_shape=jax.ShapeDtypeStruct((rows, width), jnp.bfloat16),
        compiler_params=pltpu.CompilerParams(vmem_limit_bytes=16 * MIB),
        cost_estimate=pl.CostEstimate(
            flops=rows * width * fanout * 100, bytes_accessed=rows * width * 2, transcendentals=0
        ),
        name="count_matrix",
    )(index)


def first_kernel(blocks, fanout, arrived_ref, place_ref, hot_ref, counts_ref, self_ref, neigh_ref,
                 pre_ref, stats_ref, features):
    step = pl.program_id(0)
    rows = place_ref.shape[0]

    @pl.when(step < blocks)
    def _():
        place = one_hot(place_ref[...], arrived_ref.shape[0])
        cold = jnp.dot(place, arrived_ref[...], preferred_element_type=jnp.float32)
        here = pl.ds(pl.multiple_of(step * rows, rows), rows)
        features[here, :] = cold.astype(jnp.bfloat16) + hot_ref[...]

    @pl.when(step >= blocks)
    def _():
        here = pl.ds(pl.multiple_of((step - blocks) * rows, rows), rows)
        total = jnp.dot(counts_ref[...], features[...], preferred_element_type=jnp.float32)
        mean = (total / fanout).astype(jnp.bfloat16)
        pre = jnp.dot(features[here, :], self_ref[...], preferred_element_type=jnp.float32)
        pre = pre + jnp.dot(mean, neigh_ref[...], preferred_element_type=jnp.float32)
        pre_ref[...] = pre
        both = jnp.concatenate(
            [jnp.sum(pre, axis=0, keepdims=True), jnp.sum(pre * pre, axis=0, keepdims=True)], axis=0
        )

        @pl.when(step == blocks)
        def _():
            stats_ref[...] = both

        @pl.when(step > blocks)
        def _():
            stats_ref[...] += both


def first_layer(arrived, place, hot_feat, counts, self_first, neigh_first, fanout):
    nodes, width = hot_feat.shape
    units = self_first.shape[1]
    step = block_of(nodes, 512)
    blocks = nodes // step
    early = lambda i: (jnp.minimum(i, blocks - 1), 0)
    late = lambda i: (jnp.maximum(i - blocks, 0), 0)
    return pl.pallas_call(
        functools.partial(first_kernel, blocks, fanout),
        grid=(2 * blocks,),
        in_specs=[
            whole(arrived.shape),
            pl.BlockSpec((step, place.shape[1]), early),
            pl.BlockSpec((step, width), early),
            pl.BlockSpec((step, counts.shape[1]), late),
            whole(self_first.shape),
            whole(neigh_first.shape),
        ],
        out_specs=[pl.BlockSpec((step, units), late), whole((2, units))],
        out_shape=[
            jax.ShapeDtypeStruct((nodes, units), jnp.float32),
            jax.ShapeDtypeStruct((2, units), jnp.float32),
        ],
        scratch_shapes=[pltpu.VMEM((nodes, width), jnp.bfloat16)],
        compiler_params=pltpu.CompilerParams(vmem_limit_bytes=36 * MIB),
        name="first_layer",
    )(arrived, place, hot_feat, counts, self_first, neigh_first)


def stats_kernel(hosts, within, own_ref, out_ref, near, far, part, send_near, recv_near, send_far, recv_far):
    host, lane = lax.axis_index("hst"), lax.axis_index("dev")
    barrier = pltpu.get_barrier_semaphore()
    for away in range(1, within):
        pl.semaphore_signal(barrier, inc=1, device_id={"dev": lax.rem(lane + away, within)},
                            device_id_type=pl.DeviceIdType.MESH)
    for away in range(1, hosts):
        pl.semaphore_signal(barrier, inc=1, device_id={"hst": lax.rem(host + away, hosts)},
                            device_id_type=pl.DeviceIdType.MESH)
    pl.semaphore_wait(barrier, within + hosts - 2)

    def exchange(source, slots, axis, me, size, send, recv):
        copies = []
        for away in range(1, size):
            copy = pltpu.make_async_remote_copy(
                src_ref=source, dst_ref=slots.at[away - 1], send_sem=send.at[away - 1],
                recv_sem=recv.at[away - 1], device_id={axis: lax.rem(me + away, size)},
                device_id_type=pl.DeviceIdType.MESH,
            )
            copy.start()
            copies.append(copy)
        for copy in copies:
            copy.wait()
        total = source[...]
        for away in range(1, size):
            total = total + slots[away - 1]
        return total

    part[...] = exchange(own_ref, near, "dev", lane, within, send_near, recv_near)
    out_ref[...] = exchange(part, far, "hst", host, hosts, send_far, recv_far)


def sum_stats(own, hosts, within):
    return pl.pallas_call(
        functools.partial(stats_kernel, hosts, within),
        in_specs=[pl.BlockSpec(memory_space=pltpu.VMEM)],
        out_specs=pl.BlockSpec(memory_space=pltpu.VMEM),
        out_shape=jax.ShapeDtypeStruct(own.shape, own.dtype),
        scratch_shapes=[
            pltpu.VMEM((within - 1,) + own.shape, own.dtype),
            pltpu.VMEM((hosts - 1,) + own.shape, own.dtype),
            pltpu.VMEM(own.shape, own.dtype),
            pltpu.SemaphoreType.DMA((within - 1,)),
            pltpu.SemaphoreType.DMA((within - 1,)),
            pltpu.SemaphoreType.DMA((hosts - 1,)),
            pltpu.SemaphoreType.DMA((hosts - 1,)),
        ],
        compiler_params=pltpu.CompilerParams(
            collective_id=0, has_side_effects=True, vmem_limit_bytes=4 * MIB
        ),
        name="sum_stats",
    )(own)


def norm_kernel(total_rows, pre_ref, stats_ref, gain_ref, shift_ref, picks_ref, hidden_ref, boundary_ref, held):
    step = pl.program_id(0)
    mean = stats_ref[0:1, :] / total_rows
    variance = stats_ref[1:2, :] / total_rows - mean * mean
    scale = lax.rsqrt(variance + epsilon)
    hidden = jnp.maximum((pre_ref[...] - mean) * scale * gain_ref[...] + shift_ref[...], 0.0)
    hidden = hidden.astype(jnp.bfloat16)
    hidden_ref[...] = hidden
    picks = one_hot(picks_ref[...] - step * hidden.shape[0], hidden.shape[0])
    picked = jnp.dot(picks, hidden, preferred_element_type=jnp.float32)

    @pl.when(step == 0)
    def _():
        held[...] = picked

    @pl.when(step > 0)
    def _():
        held[...] += picked

    @pl.when(step == pl.num_programs(0) - 1)
    def _():
        boundary_ref[...] = held[...].astype(jnp.bfloat16)


def norm_layer(pre, stats, gain, shift, picks, total_rows):
    nodes, units = pre.shape
    step = block_of(nodes, 512)
    edge = picks.shape[0]
    return pl.pallas_call(
        functools.partial(norm_kernel, total_rows),
        grid=(nodes // step,),
        in_specs=[
            pl.BlockSpec((step, units), lambda i: (i, 0)),
            whole(stats.shape),
            whole((1, units)),
            whole((1, units)),
            whole((edge, 1)),
        ],
        out_specs=[pl.BlockSpec((step, units), lambda i: (i, 0)), whole((edge, units))],
        out_shape=[
            jax.ShapeDtypeStruct((nodes, units), jnp.bfloat16),
            jax.ShapeDtypeStruct((edge, units), jnp.bfloat16),
        ],
        scratch_shapes=[pltpu.VMEM((edge, units), jnp.float32)],
        compiler_params=pltpu.CompilerParams(vmem_limit_bytes=20 * MIB),
        name="norm_layer",
    )(pre, stats, gain[None, :], shift[None, :], picks)


def last_kernel(within, fanout, boundary_ref, hidden_ref, counts_ref, self_ref, neigh_ref, out_ref,
                received, send, recv, own_sem):
    lane = lax.axis_index("dev")
    nodes = hidden_ref.shape[0]
    targets = counts_ref.shape[0]
    slots = boundary_ref.shape[0] // within
    barrier = pltpu.get_barrier_semaphore()
    for away in range(1, within):
        pl.semaphore_signal(barrier, inc=1, device_id={"dev": lax.rem(lane + away, within)},
                            device_id_type=pl.DeviceIdType.MESH)
    pl.semaphore_wait(barrier, within - 1)
    mine = pl.ds(pl.multiple_of(lane * slots, slots), slots)
    copies = []
    for away in range(1, within):
        peer = lax.rem(lane + away, within)
        copy = pltpu.make_async_remote_copy(
            src_ref=boundary_ref.at[pl.ds(pl.multiple_of(peer * slots, slots), slots)],
            dst_ref=received.at[mine],
            send_sem=send.at[away - 1], recv_sem=recv.at[away - 1], device_id={"dev": peer},
            device_id_type=pl.DeviceIdType.MESH,
        )
        copy.start()
        copies.append(copy)
    own = pltpu.make_async_copy(boundary_ref.at[mine], received.at[mine], own_sem)
    own.start()
    total = jnp.dot(counts_ref[:, :nodes], hidden_ref[...], preferred_element_type=jnp.float32)
    scores = jnp.dot(hidden_ref[:targets, :], self_ref[...], preferred_element_type=jnp.float32)
    own.wait()
    for copy in copies:
        copy.wait()
    total = total + jnp.dot(counts_ref[:, nodes:], received[...], preferred_element_type=jnp.float32)
    mean = (total / fanout).astype(jnp.bfloat16)
    out_ref[...] = scores + jnp.dot(mean, neigh_ref[...], preferred_element_type=jnp.float32)


def last_layer(boundary, hidden, counts, self_second, neigh_second, within, fanout):
    return pl.pallas_call(
        functools.partial(last_kernel, within, fanout),
        in_specs=[pl.BlockSpec(memory_space=pltpu.VMEM)] * 5,
        out_specs=pl.BlockSpec(memory_space=pltpu.VMEM),
        out_shape=jax.ShapeDtypeStruct((counts.shape[0], self_second.shape[1]), jnp.float32),
        scratch_shapes=[
            pltpu.VMEM(boundary.shape, boundary.dtype),
            pltpu.SemaphoreType.DMA((within - 1,)),
            pltpu.SemaphoreType.DMA((within - 1,)),
            pltpu.SemaphoreType.DMA,
        ],
        compiler_params=pltpu.CompilerParams(
            collective_id=1, has_side_effects=True, vmem_limit_bytes=24 * MIB
        ),
        name="last_layer",
    )(boundary, hidden, counts, self_second, neigh_second)


def local(
    hot_rows,
    cold_rows,
    hot_mask,
    hot_id,
    cold_owner,
    cold_pos,
    cold_send,
    adjacency_one,
    adjacency_two,
    halo_send,
    self_first,
    neigh_first,
    bn_gain,
    bn_shift,
    self_second,
    neigh_second,
):
    hosts = lax.axis_size("hst")
    within = lax.axis_size("dev")
    nodes = hot_mask.shape[0]
    outgoing = select_rows(cold_rows, cold_send[0])
    slots = outgoing.shape[0] // (hosts * within)
    arrived = lax.all_to_all(outgoing, ("hst", "dev"), split_axis=0, concat_axis=0, tiled=True)

    hot_feat = jnp.where(
        hot_mask[:, None] == 1, hot_rows.at[hot_id].get(mode="promise_in_bounds"), 0
    )
    source = jnp.where(hot_mask == 1, -1, cold_owner * slots + cold_pos)
    place = source[:, None]
    counts_one = count_matrix(adjacency_one, nodes)
    counts_two = count_matrix(adjacency_two, nodes + halo_send.shape[1])
    picks = halo_send[0][:, None]

    pre, own = first_layer(
        arrived, place, hot_feat, counts_one, self_first, neigh_first, adjacency_one.shape[1]
    )
    stats = sum_stats(own, hosts, within)
    hidden, boundary = norm_layer(pre, stats, bn_gain, bn_shift, picks, nodes * hosts * within)
    return last_layer(
        boundary, hidden, counts_two, self_second, neigh_second, within, adjacency_two.shape[1]
    )


def solution(mesh):
    placed = (
        P(),
        P(("hst", "dev"), None),
        P(("hst", "dev")),
        P(("hst", "dev")),
        P(("hst", "dev")),
        P(("hst", "dev")),
        P(("hst", "dev"), None),
        P(("hst", "dev"), None),
        P(("hst", "dev"), None),
        P(("hst", "dev"), None),
        P(),
        P(),
        P(),
        P(),
        P(),
        P(),
    )
    return jax.shard_map(
        local, mesh=mesh, in_specs=placed, out_specs=P(("hst", "dev"), None), check_vma=False
    )
```
